32 devices in a mesh: gx: 4 (over x, core), gy: 8 (over z, y).
Axes of the slice: x: 2, y: 2, z: 4, core: 2. Of those that a mesh axis runs over, the one named last changes fastest.
Arguments:
- log_crit: float32 [512, 512, 128], P('gx', 'gy'), may hold values from -4 to 4
- col_bins: int32 [512, 512, 4], P('gx', 'gy'), may hold values from 0 to 127
- rate_table: bfloat16 [128, 64], replicated, may hold values from 0.0039978027 to 0.059814453
- tile_mask: int32 [16, 16, 4], P('gx', 'gy'), may hold values from 0 to 1, as said below
- tile_route: int32 [16, 16, 4], P('gx', 'gy'), may hold values from 0 to 7, as said below
- filt_x: float32 [512], replicated, may hold values from 0.1 to 1, as said below
- filt_y: float32 [512], replicated, may hold values from 0.1 to 1, as said below
Outputs:
- recomb: float32 [512, 512, 128], P('gx', 'gy')
- smoothed: float32 [512, 512, 128], P('gx', 'gy')
- load: float32 [4, 8], P('gx', 'gy')
The draws below stay inside these ranges and needn't reach their ends.
Inputs may be any that keep to these rules, and one draw needn't show every extreme that they name: `tile_mask`: tiles form blocks of 4 x 2 x 4 (indices a // 4, b // 2); among the blocks with the same a // 4, some block has all 32 tiles active. `tile_route`: counting only tiles with tile_mask 1: among the blocks with the same a // 4 at most 16 active tiles share a route, and in every draw some such row of blocks gives every route exactly 16; at most 4 active tiles of one block share a route, and in every draw some block has 4 that do. filt_x[m] == filt_x[512 - m] for 0 < m < 512. filt_y[n] == filt_y[512 - n] for 0 < n < 512.
All inputs are finite; a program needn't handle non-finite values.
Results may differ from the reference program's by a relative error of at most 0.0003.
Values sent between devices are 32-bit elements; how exact they have to be, the bound alone decides.
A program may use at most 128 MiB of HBM per device.

```python
import math
import jax
import jax.numpy as jnp
from jax import lax

TE = 32
TX = 4
TY = 2
TZ = 4
BINS = 128
NODES = 64
RECV = 16
NX = 512
NY = 512
NZ = 128
N_GX = 4
N_GY = 8


def tile_plan(key):
    base_key = jax.random.fold_in(key, 11)
    k_count, k_busy, k_row, k_perm, k_spare = jax.random.split(base_key, 5)
    tiles_block = TX * TY * TZ
    half_tiles = tiles_block // 2
    quarter_tiles = tiles_block // 4
    pair_cap = tiles_block // N_GY
    counts = jax.random.randint(k_count, (N_GX, N_GY), quarter_tiles, half_tiles)
    busiest = jax.random.randint(k_busy, (N_GX,), 0, N_GY)
    full_row = jax.random.randint(k_row, (), 0, N_GX)
    column_ids = jnp.arange(N_GY)[None, :]
    counts = jnp.where(jnp.arange(N_GX)[:, None] == full_row, half_tiles, counts)
    counts = jnp.where(column_ids == busiest[:, None], tiles_block, counts)
    counts = jnp.where(column_ids == (busiest[:, None] + 1) % N_GY, 0, counts)
    perm_keys = jax.random.split(k_perm, N_GX * N_GY)
    tile_ranks = jax.vmap(lambda sub_key: jax.random.permutation(sub_key, tiles_block))(perm_keys).reshape(N_GX, N_GY, tiles_block)
    active = (tile_ranks < counts[:, :, None]).astype(jnp.int32)
    row_flags = active.reshape(N_GX, N_GY * tiles_block)
    before = jnp.cumsum(row_flags, axis=1) - row_flags
    chosen = (before // pair_cap % N_GY).reshape(N_GX, N_GY, tiles_block)
    spare_route = jax.random.randint(k_spare, (N_GX, N_GY, tiles_block), 0, N_GY)
    routes = jnp.where(active == 1, chosen, spare_route).astype(jnp.int32)
    return (lay_out(active), lay_out(routes))


def lay_out(values):
    shaped = values.reshape(N_GX, N_GY, TX, TY, TZ).transpose(0, 2, 1, 3, 4)
    return shaped.reshape(N_GX * TX, N_GY * TY, TZ)


def window_draw(key, length):
    half = length // 2 + 1
    values = jnp.exp(jax.random.uniform(key, (half,), jnp.float32, math.log(0.1), 0.0))
    indices = jnp.arange(length)
    folded = jnp.minimum(indices, length - indices)
    return values[folded].astype(jnp.float32)


def draw_tile_mask(key, part):
    return tile_plan(key)[0]


def draw_tile_route(key, part):
    return tile_plan(key)[1]


def draw_filt_x(key, part):
    return window_draw(jax.random.fold_in(key, 21), NX)


def draw_filt_y(key, part):
    return window_draw(jax.random.fold_in(key, 23), NY)


def plant(result, own_key, smallest, largest):
    place = [jax.random.randint(jax.random.fold_in(own_key, axis), (), 0, length) for axis, length in enumerate(result.shape)]
    widest = result.shape.index(max(result.shape))
    beside = place[:widest] + [(place[widest] + 1) % result.shape[widest]] + place[widest + 1:]
    return result.at[tuple(place)].set(smallest).at[tuple(beside)].set(largest)


def block_scale(stream_key, dims, shards, low, largest):
    loudness = 1.0
    for position, parts in shards:
        heights = jax.random.uniform(jax.random.fold_in(jax.random.fold_in(stream_key, 6), position), (parts,), jnp.float32, low / len(shards), largest / len(shards))
        loudness = loudness * jnp.repeat(jnp.exp(heights), dims[position] // parts).reshape((-1,) + (1,) * (len(dims) - 1 - position))
    return loudness


def normal_values(own_key, shape, scale, reach, cuts=(), kind=jnp.bfloat16):
    drawn = scale * jax.random.normal(own_key, shape, jnp.float32)
    if cuts:
        drawn = drawn * block_scale(own_key, shape, cuts, -0.22, 0.18)
    return jnp.clip(drawn, -reach, reach).astype(kind)


def setup_inputs(seed: int = 0) -> dict:
    key_of = jax.random.split(jax.random.key(seed), 8)
    return {
        "log_crit": normal_values(key_of[0], (NX, NY, NZ), 1.0, 4.0, ((0, 4), (1, 8)), jnp.float32),
        "col_bins": plant(jax.random.randint(key_of[1], (NX, NY, TZ), 0, BINS), jax.random.fold_in(key_of[1], 1), 0, BINS - 1).astype(jnp.int32),
        "rate_table": jnp.clip(jnp.exp(jax.random.uniform(key_of[2], (BINS, NODES), jnp.float32, math.log(0.0039978027), math.log(0.059814453))), 0.0039978027, 0.059814453).astype(jnp.bfloat16),
        "tile_mask": draw_tile_mask(jax.random.fold_in(key_of[7], 71), 0),
        "tile_route": draw_tile_route(jax.random.fold_in(key_of[7], 71), 0),
        "filt_x": draw_filt_x(jax.random.fold_in(key_of[7], 71), 0),
        "filt_y": draw_filt_y(jax.random.fold_in(key_of[7], 71), 0),
    }


steepness = 3.0


def reference(log_crit, col_bins, rate_table, tile_mask, tile_route, filt_x, filt_y):
    size_x, size_y, size_z = log_crit.shape
    rows_x = N_GX * TX
    rows_y = N_GY * TY
    tile_cells = log_crit.reshape(rows_x, TE, rows_y, TE, TZ, TE).transpose(0, 2, 4, 1, 3, 5).reshape(-1, TE, TE, TE)
    tile_bins = col_bins.reshape(rows_x, TE, rows_y, TE, TZ).transpose(0, 2, 4, 1, 3).reshape(-1, TE, TE)
    live_flags = tile_mask.reshape(-1)
    table_f32 = rate_table.astype(jnp.float32)
    node_grid = -2.5 + 5.0 * jnp.arange(NODES, dtype=jnp.float32) / (NODES - 1)

    def tile_value(operands):
        field, bin_cols, is_live = operands
        table_rows = table_f32[bin_cols]

        def active(unused):
            cutoff = jax.nn.sigmoid((field[..., None] - node_grid) * steepness)
            return jnp.sum(cutoff * table_rows[:, :, None, :], axis=-1)

        def quiet(unused):
            return jnp.zeros_like(field)

        return lax.cond(is_live == 1, active, quiet, 0)

    values = lax.map(tile_value, (tile_cells, tile_bins, live_flags))
    tile_mean = jnp.mean(values.reshape(values.shape[0], -1), axis=1).reshape(rows_x, rows_y, TZ)
    onehot = (tile_route[..., None] == jnp.arange(N_GY)).astype(jnp.float32)
    per_row = jnp.einsum('abt,abtg->ag', tile_mean.astype(jnp.float32), onehot)
    load = jnp.sum(per_row.reshape(N_GX, TX, N_GY), axis=1) / RECV
    recomb = values.reshape(rows_x, rows_y, TZ, TE, TE, TE).transpose(0, 3, 1, 4, 2, 5).reshape(size_x, size_y, size_z)
    gain_plane = filt_x[:, None, None] * filt_y[None, :, None]
    z_block = 16 if size_z % 16 == 0 else size_z
    blocks = recomb.reshape(size_x, size_y, size_z // z_block, z_block).transpose(2, 0, 1, 3)

    def smooth_block(block):
        spectrum = jnp.fft.fft2(block, axes=(0, 1))
        return jnp.real(jnp.fft.ifft2(spectrum * gain_plane, axes=(0, 1))).astype(jnp.float32)

    smoothed = lax.map(smooth_block, blocks).transpose(1, 2, 0, 3).reshape(size_x, size_y, size_z)
    return recomb, smoothed, load
```

```python
import functools
import math

import jax
import jax.numpy as jnp
from jax import lax
from jax.experimental import pallas as pl
from jax.experimental.pallas import tpu as pltpu
from jax.sharding import PartitionSpec as P

steepness = 3.0
vmem_grant = 60 * 1024 * 1024
MESH = pl.DeviceIdType.MESH


def node_growth(nodes):
    return [math.exp(steepness * (-2.5 + 5.0 * q / (nodes - 1))) for q in range(nodes // 2, nodes)]


def join(left, right):
    num_left, den_left = left
    num_right, den_right = right
    return (num_left * den_right + num_right * den_left, den_left * den_right)


def integral(field, upper, lower, growth, scratch_a, scratch_b):
    pairs = len(growth)
    v = jnp.exp(field * steepness)
    y = v + jnp.exp(field * -steepness)
    scratch_a[...] = upper + lower
    position = lax.broadcasted_iota(jnp.int32, upper.shape, 0).astype(jnp.float32)
    step = math.log(growth[1] / growth[0])
    rise = jnp.exp(position * step + math.log(growth[0]))
    fall = jnp.exp(position * -step - math.log(growth[0]))
    scratch_b[...] = upper * fall + lower * rise
    total = None
    for first in range(0, pairs, 4):
        terms = []
        for p in range(first, min(first + 4, pairs)):
            num = scratch_a[pl.ds(p, 1), :] * v + scratch_b[pl.ds(p, 1), :]
            terms.append((num, y + (growth[p] + 1.0 / growth[p])))
        while len(terms) > 1:
            terms = [
                join(terms[i], terms[i + 1]) if i + 1 < len(terms) else terms[i]
                for i in range(0, len(terms), 2)
            ]
        part = terms[0][0] * (1.0 / terms[0][1])
        total = part if total is None else total + part
    return total


def eval_kernel(
    growth, tiles, field_ref, bins_ref, live_ref, table_ref, recomb_ref, zfirst_ref, sums_ref,
    turned, values, scratch_a, scratch_b,
):
    cells_x, rows, depth_all = field_ref.shape
    edge = depth_all // tiles
    pairs = len(growth)
    bins_total = table_ref.shape[1]
    for row in range(rows):
        turned[row] = field_ref[:, row, :].T

    def step(i, carry):
        row, tile = i // tiles, i % tiles
        span = pl.ds(pl.multiple_of(tile * edge, edge), edge)
        levels = lax.broadcasted_iota(jnp.int32, (bins_total, cells_x), 0)
        onehot = jnp.where(levels == bins_ref[pl.ds(i, 1), :], 1.0, 0.0).astype(jnp.bfloat16)
        rows_here = jnp.dot(table_ref[...], onehot, preferred_element_type=jnp.float32)
        rows_here = rows_here * live_ref[pl.ds(i, 1), :]
        out = integral(
            turned[row, span, :], rows_here[:pairs], rows_here[pairs:], growth, scratch_a, scratch_b
        )
        values[row, span, :] = out
        sums_ref[pl.ds(i, 1), :] = jnp.sum(out, axis=0, keepdims=True)
        return carry

    lax.fori_loop(0, rows * tiles, step, 0)
    for row in range(rows):
        recomb_ref[:, row, :] = values[row].T
        zfirst_ref[:, row, :] = values[row]


def evaluate(log_crit, bins, live, table, growth, tiles):
    cells_x, cells_y, depth_all = log_crit.shape
    rows = 8
    nodes, bins_total = table.shape
    return pl.pallas_call(
        functools.partial(eval_kernel, growth, tiles),
        grid=(cells_y // rows,),
        in_specs=[
            pl.BlockSpec((cells_x, rows, depth_all), lambda j: (0, j, 0)),
            pl.BlockSpec((rows * tiles, cells_x), lambda j: (j, 0)),
            pl.BlockSpec((rows * tiles, cells_x), lambda j: (j, 0)),
            pl.BlockSpec((nodes, bins_total), lambda j: (0, 0)),
        ],
        out_specs=[
            pl.BlockSpec((cells_x, rows, depth_all), lambda j: (0, j, 0)),
            pl.BlockSpec((depth_all, rows, cells_x), lambda j: (0, j, 0)),
            pl.BlockSpec((rows * tiles, cells_x), lambda j: (j, 0)),
        ],
        out_shape=[
            jax.ShapeDtypeStruct((cells_x, cells_y, depth_all), jnp.float32),
            jax.ShapeDtypeStruct((depth_all, cells_y, cells_x), jnp.float32),
            jax.ShapeDtypeStruct((cells_y * tiles, cells_x), jnp.float32),
        ],
        scratch_shapes=[
            pltpu.VMEM((rows, depth_all, cells_x), jnp.float32),
            pltpu.VMEM((rows, depth_all, cells_x), jnp.float32),
            pltpu.VMEM((nodes // 2, cells_x), jnp.float32),
            pltpu.VMEM((nodes // 2, cells_x), jnp.float32),
        ],
        compiler_params=pltpu.CompilerParams(vmem_limit_bytes=vmem_grant),
        name="evaluate",
    )(log_crit, bins, live, table)


def halves(value):
    high = value.astype(jnp.bfloat16)
    return high, (value - high.astype(jnp.float32)).astype(jnp.bfloat16)


def outer_halves(value):
    high = lax.reduce_precision(value, 8, 7)
    low = lax.reduce_precision(value - high, 8, 7)
    return high.astype(jnp.bfloat16), low.astype(jnp.bfloat16)


def dot3(a_high, a_low, b_high, b_low):
    dot = functools.partial(jnp.dot, preferred_element_type=jnp.float32)
    return dot(a_high, b_high) + (dot(a_high, b_low) + dot(a_low, b_high))


def smooth_kernel(
    span_x, span_y, zfirst, cy_high, cy_low, cx_high, cx_low, out,
    plane, done, high, low, send_sem, recv_sem, own_sem, back_send, back_recv, back_own,
):
    planes, devices, cells_y, cells_x = zfirst.shape
    size_y, size_x = high.shape
    block = 128 if size_y % 128 == 0 else size_y
    gx, gy = lax.axis_index("gx"), lax.axis_index("gy")
    me = gx * span_y + gy

    def at(i, j):
        return {"gx": i, "gy": j}

    def place(ref, k, i, j):
        return ref.at[
            k,
            pl.ds(pl.multiple_of(j * cells_y, cells_y), cells_y),
            pl.ds(pl.multiple_of(i * cells_x, cells_x), cells_x),
        ]

    def each_peer(act):
        def body(n, carry):
            offset_y, offset_x = n // span_x, n % span_x
            act(lax.rem(gx + offset_x, span_x), lax.rem(gy + offset_y, span_y))
            return carry

        lax.fori_loop(1, devices, body, 0)

    barrier = pltpu.get_barrier_semaphore()
    each_peer(
        lambda i, j: pl.semaphore_signal(barrier, inc=1, device_id=at(i, j), device_id_type=MESH)
    )
    for k in range(planes):
        pltpu.make_async_copy(zfirst.at[k, me], place(plane, k, gx, gy), own_sem.at[k]).start()
    pl.semaphore_wait(barrier, devices - 1)

    def send_plane(k):
        def act(i, j):
            pltpu.make_async_remote_copy(
                src_ref=zfirst.at[k, i * span_y + j],
                dst_ref=place(plane, k, gx, gy),
                send_sem=send_sem.at[k],
                recv_sem=recv_sem.at[k],
                device_id=at(i, j),
                device_id_type=MESH,
            ).start()

        each_peer(act)

    def send_back(k):
        def act(i, j):
            pltpu.make_async_remote_copy(
                src_ref=place(done, k, i, j),
                dst_ref=out.at[k, me],
                send_sem=back_send.at[k],
                recv_sem=back_recv.at[k],
                device_id=at(i, j),
                device_id_type=MESH,
            ).start()

        each_peer(act)
        pltpu.make_async_copy(place(done, k, gx, gy), out.at[k, me], back_own.at[k]).start()

    def wait_others(sem, k):
        some = zfirst.at[0, pl.ds(0, devices - 1)]
        pltpu.make_async_copy(some, some, sem.at[k]).wait()

    def wait_own(sem, k):
        one = zfirst.at[0, 0]
        pltpu.make_async_copy(one, one, sem.at[k]).wait()

    for k in range(planes):
        send_plane(k)

    def finish_plane(k, carry):
        wait_own(own_sem, k)
        wait_others(recv_sem, k)

        def split(r, carry):
            rows = pl.ds(pl.multiple_of(r * block, block), block)
            high[rows, :], low[rows, :] = halves(plane[k, rows, :])
            return carry

        lax.fori_loop(0, size_y // block, split, 0)

        def multiply(r, carry):
            rows = pl.ds(pl.multiple_of(r * block, block), block)
            along_y = dot3(cy_high[rows, :], cy_low[rows, :], high[...], low[...])
            y_high, y_low = halves(along_y)
            done[k, rows, :] = dot3(y_high, y_low, cx_high[...], cx_low[...])
            return carry

        lax.fori_loop(0, size_y // block, multiply, 0)
        send_back(k)
        return carry

    lax.fori_loop(0, planes, finish_plane, 0)
    for k in range(planes):
        wait_others(send_sem, k)
        wait_others(back_send, k)
        wait_own(back_own, k)
        wait_others(back_recv, k)


def smooth(zfirst, cy, cx, span_x, span_y):
    planes, devices, cells_y, cells_x = zfirst.shape
    size_y, size_x = cy.shape[0], cx.shape[0]
    anywhere = pl.BlockSpec(memory_space=pl.ANY)
    inside = pl.BlockSpec(memory_space=pltpu.VMEM)
    sems = pltpu.SemaphoreType.DMA((planes,))
    return pl.pallas_call(
        functools.partial(smooth_kernel, span_x, span_y),
        in_specs=[anywhere] + [inside] * 4,
        out_specs=anywhere,
        out_shape=jax.ShapeDtypeStruct(zfirst.shape, jnp.float32),
        scratch_shapes=[
            pltpu.VMEM((planes, size_y, size_x), jnp.float32),
            pltpu.VMEM((planes, size_y, size_x), jnp.float32),
            pltpu.VMEM((size_y, size_x), jnp.bfloat16),
            pltpu.VMEM((size_y, size_x), jnp.bfloat16),
        ]
        + [sems] * 6,
        compiler_params=pltpu.CompilerParams(
            collective_id=0, has_side_effects=True, vmem_limit_bytes=vmem_grant
        ),
        name="smooth",
    )(zfirst, *outer_halves(cy), *outer_halves(cx))


def turn_kernel(source_ref, out_ref):
    for row in range(source_ref.shape[1]):
        out_ref[:, row, :] = source_ref[:, row, :].T


def turn(source):
    depth_all, cells_y, cells_x = source.shape
    rows = 8
    return pl.pallas_call(
        turn_kernel,
        grid=(cells_y // rows,),
        in_specs=[pl.BlockSpec((depth_all, rows, cells_x), lambda j: (0, j, 0))],
        out_specs=pl.BlockSpec((cells_x, rows, depth_all), lambda j: (0, j, 0)),
        out_shape=jax.ShapeDtypeStruct((cells_x, cells_y, depth_all), jnp.float32),
        name="turn",
    )(source)


def circulant(gain):
    length = gain.shape[0]
    half = length // 2
    indices = jnp.arange(length, dtype=jnp.int32)
    freq = jnp.concatenate(
        [jnp.arange(half + 1, dtype=jnp.int32), jnp.arange(1, half, dtype=jnp.int32)]
    )
    angles = (
        2.0 * math.pi / length * (indices[:, None] * freq[None, :] % length).astype(jnp.float32)
    )
    table = jnp.where(indices[None, :] < half + 1, jnp.cos(angles), jnp.sin(angles))
    weight = jnp.concatenate([gain[: half + 1], gain[1:half]])
    doubled = jnp.where((freq == 0) | (freq == half), 1.0, 2.0).astype(jnp.float32)
    return jnp.dot(
        table * (weight * doubled / length), table.T, precision=lax.Precision.HIGHEST
    )


def on_device(log_crit, col_bins, rate_table, tile_mask, tile_route, filt_x, filt_y):
    blocks_x, blocks_y, tiles = tile_mask.shape
    cells_x, cells_y, depth_all = log_crit.shape
    edge = cells_x // blocks_x
    span_x, span_y = lax.axis_size("gx"), lax.axis_size("gy")
    devices = span_x * span_y
    nodes = rate_table.shape[1]
    half = nodes // 2

    bins = col_bins.transpose(1, 2, 0).reshape(cells_y * tiles, cells_x)
    live = (tile_mask == 1).astype(jnp.float32).transpose(1, 2, 0)
    live = jnp.broadcast_to(
        live[:, None, :, :, None], (blocks_y, edge, tiles, blocks_x, edge)
    ).reshape(cells_y * tiles, cells_x)
    table = jnp.concatenate([rate_table[:, half:], rate_table[:, half - 1 :: -1]], axis=1).T

    recomb, zfirst, sums = evaluate(log_crit, bins, live, table, node_growth(nodes), tiles)

    tile_means = jnp.sum(
        sums.reshape(blocks_y, edge, tiles, blocks_x, edge), axis=(1, 4)
    ) / (edge * edge * edge)
    route = tile_route.transpose(1, 2, 0)
    capacity = blocks_x * blocks_y * tiles // 2
    route_ids = jnp.arange(span_y, dtype=jnp.int32)
    contribution = (
        jnp.sum(
            jnp.where(route[..., None] == route_ids, tile_means[..., None], 0.0), axis=(0, 1, 2)
        )
        / capacity
    )
    device_load = lax.psum_scatter(contribution, "gy", scatter_dimension=0, tiled=True)[0]

    back = smooth(
        zfirst.reshape(depth_all // devices, devices, cells_y, cells_x),
        circulant(filt_y), circulant(filt_x), span_x, span_y,
    )
    smoothed = turn(back.reshape(depth_all, cells_y, cells_x))
    return (recomb, smoothed, device_load.reshape(1, 1))


def solution(mesh):
    placed = (
        P("gx", "gy", None),
        P("gx", "gy", None),
        P(),
        P("gx", "gy", None),
        P("gx", "gy", None),
        P(),
        P(),
    )
    return jax.shard_map(
        on_device,
        mesh=mesh,
        in_specs=placed,
        out_specs=(P("gx", "gy", None), P("gx", "gy", None), P("gx", "gy")),
        check_vma=False,
    )
```

```python
import functools
import math

import jax
import jax.numpy as jnp
from jax import lax
from jax.experimental import pallas as pl
from jax.experimental.pallas import tpu as pltpu
from jax.sharding import PartitionSpec as P

steepness = 3.0
vmem_grant = 60 * 1024 * 1024
MESH = pl.DeviceIdType.MESH


def node_growth(nodes):
    return [math.exp(steepness * (-2.5 + 5.0 * q / (nodes - 1))) for q in range(nodes // 2, nodes)]


def join(left, right):
    num_left, den_left = left
    num_right, den_right = right
    return (num_left * den_right + num_right * den_left, den_left * den_right)


def integral(field, i, growth, coef_a, coef_b):
    pairs = len(growth)
    v = jnp.exp(field * steepness)
    y = v + jnp.exp(field * -steepness)
    total = None
    for first in range(0, pairs, 4):
        terms = []
        for p in range(first, min(first + 4, pairs)):
            num = coef_a[i, pl.ds(p, 1), :] * v + coef_b[i, pl.ds(p, 1), :]
            terms.append((num, y + (growth[p] + 1.0 / growth[p])))
        while len(terms) > 1:
            terms = [
                join(terms[i], terms[i + 1]) if i + 1 < len(terms) else terms[i]
                for i in range(0, len(terms), 2)
            ]
        part = terms[0][0] * (1.0 / terms[0][1])
        total = part if total is None else total + part
    return total


def eval_kernel(
    growth, tiles, field_ref, bins_ref, live_ref, table_ref, rise_ref, recomb_ref, zfirst_ref,
    sums_ref, turned, values, coef_a, coef_b,
):
    cells_x, rows, depth_all = field_ref.shape
    edge = depth_all // tiles
    pairs = len(growth)
    bins_total = table_ref.shape[1]
    for row in range(rows):
        turned[row] = field_ref[:, row, :].T

    def gather(i, carry):
        levels = lax.broadcasted_iota(jnp.int32, (bins_total, cells_x), 0)
        onehot = jnp.where(levels == bins_ref[pl.ds(i, 1), :], 1.0, 0.0).astype(jnp.bfloat16)
        rows_here = jnp.dot(table_ref[...], onehot, preferred_element_type=jnp.float32)
        rows_here = rows_here * live_ref[pl.ds(i, 1), :]
        upper, lower = rows_here[:pairs], rows_here[pairs:]
        coef_a[i] = upper + lower
        coef_b[i] = upper * rise_ref[1] + lower * rise_ref[0]
        return carry

    def step(i, carry):
        row, tile = i // tiles, i % tiles
        span = pl.ds(pl.multiple_of(tile * edge, edge), edge)
        out = integral(turned[row, span, :], i, growth, coef_a, coef_b)
        values[row, span, :] = out
        sums_ref[pl.ds(i, 1), :] = jnp.sum(out, axis=0, keepdims=True)
        return carry

    lax.fori_loop(0, rows * tiles, gather, 0, unroll=8)
    lax.fori_loop(0, rows * tiles, step, 0)
    for row in range(rows):
        recomb_ref[:, row, :] = values[row].T
        zfirst_ref[:, row, :] = values[row]


def evaluate(log_crit, bins, live, table, growth, tiles):
    cells_x, cells_y, depth_all = log_crit.shape
    rows = 8
    nodes, bins_total = table.shape
    ends = jnp.array([growth, [1.0 / e for e in growth]], jnp.float32)
    rise = jnp.broadcast_to(ends[:, :, None], (2, nodes // 2, cells_x))
    return pl.pallas_call(
        functools.partial(eval_kernel, growth, tiles),
        grid=(cells_y // rows,),
        in_specs=[
            pl.BlockSpec((cells_x, rows, depth_all), lambda j: (0, j, 0)),
            pl.BlockSpec((rows * tiles, cells_x), lambda j: (j, 0)),
            pl.BlockSpec((rows * tiles, cells_x), lambda j: (j, 0)),
            pl.BlockSpec((nodes, bins_total), lambda j: (0, 0)),
            pl.BlockSpec((2, nodes // 2, cells_x), lambda j: (0, 0, 0)),
        ],
        out_specs=[
            pl.BlockSpec((cells_x, rows, depth_all), lambda j: (0, j, 0)),
            pl.BlockSpec((depth_all, rows, cells_x), lambda j: (0, j, 0)),
            pl.BlockSpec((rows * tiles, cells_x), lambda j: (j, 0)),
        ],
        out_shape=[
            jax.ShapeDtypeStruct((cells_x, cells_y, depth_all), jnp.float32),
            jax.ShapeDtypeStruct((depth_all, cells_y, cells_x), jnp.float32),
            jax.ShapeDtypeStruct((cells_y * tiles, cells_x), jnp.float32),
        ],
        scratch_shapes=[
            pltpu.VMEM((rows, depth_all, cells_x), jnp.float32),
            pltpu.VMEM((rows, depth_all, cells_x), jnp.float32),
            pltpu.VMEM((rows * tiles, nodes // 2, cells_x), jnp.float32),
            pltpu.VMEM((rows * tiles, nodes // 2, cells_x), jnp.float32),
        ],
        compiler_params=pltpu.CompilerParams(vmem_limit_bytes=vmem_grant),
        name="evaluate",
    )(log_crit, bins, live, table, rise)


def halves(value):
    high = value.astype(jnp.bfloat16)
    return high, (value - high.astype(jnp.float32)).astype(jnp.bfloat16)


def outer_halves(value):
    high = lax.reduce_precision(value, 8, 7)
    low = lax.reduce_precision(value - high, 8, 7)
    return high.astype(jnp.bfloat16), low.astype(jnp.bfloat16)


def dot3(a_high, a_low, b_high, b_low):
    dot = functools.partial(jnp.dot, preferred_element_type=jnp.float32)
    return dot(a_high, b_high) + (dot(a_high, b_low) + dot(a_low, b_high))


def smooth_kernel(
    span_x, span_y, zfirst, loads, cy_high, cy_low, cx_high, cx_low, out, load_parts,
    plane, done, high, low, send_sem, recv_sem, own_sem, back_send, back_recv, back_own,
    load_sems,
):
    planes, devices, cells_y, cells_x = zfirst.shape
    size_y, size_x = high.shape
    block = 128 if size_y % 128 == 0 else size_y
    gx, gy = lax.axis_index("gx"), lax.axis_index("gy")
    me = gx * span_y + gy

    def at(i, j):
        return {"gx": i, "gy": j}

    def place(ref, k, i, j):
        return ref.at[
            k,
            pl.ds(pl.multiple_of(j * cells_y, cells_y), cells_y),
            pl.ds(pl.multiple_of(i * cells_x, cells_x), cells_x),
        ]

    def each_peer(act):
        def body(n, carry):
            offset_y, offset_x = n // span_x, n % span_x
            act(lax.rem(gx + offset_x, span_x), lax.rem(gy + offset_y, span_y))
            return carry

        lax.fori_loop(1, devices, body, 0)

    barrier = pltpu.get_barrier_semaphore()
    each_peer(
        lambda i, j: pl.semaphore_signal(barrier, inc=1, device_id=at(i, j), device_id_type=MESH)
    )
    for k in range(planes):
        pltpu.make_async_copy(zfirst.at[k, me], place(plane, k, gx, gy), own_sem.at[k]).start()
    pl.semaphore_wait(barrier, devices - 1)

    def send_plane(k):
        def act(i, j):
            pltpu.make_async_remote_copy(
                src_ref=zfirst.at[k, i * span_y + j],
                dst_ref=place(plane, k, gx, gy),
                send_sem=send_sem.at[k],
                recv_sem=recv_sem.at[k],
                device_id=at(i, j),
                device_id_type=MESH,
            ).start()

        each_peer(act)

    def send_back(k):
        def act(i, j):
            pltpu.make_async_remote_copy(
                src_ref=place(done, k, i, j),
                dst_ref=out.at[k, me],
                send_sem=back_send.at[k],
                recv_sem=back_recv.at[k],
                device_id=at(i, j),
                device_id_type=MESH,
            ).start()

        each_peer(act)
        pltpu.make_async_copy(place(done, k, gx, gy), out.at[k, me], back_own.at[k]).start()

    def wait_others(sem, k):
        some = zfirst.at[0, pl.ds(0, devices - 1)]
        pltpu.make_async_copy(some, some, sem.at[k]).wait()

    def wait_own(sem, k):
        one = zfirst.at[0, 0]
        pltpu.make_async_copy(one, one, sem.at[k]).wait()

    own_load = pltpu.make_async_copy(loads.at[gy], load_parts.at[gy], load_sems.at[2])
    own_load.start()

    def send_load(n, carry):
        j = lax.rem(gy + n, span_y)
        pltpu.make_async_remote_copy(
            src_ref=loads.at[j],
            dst_ref=load_parts.at[gy],
            send_sem=load_sems.at[0],
            recv_sem=load_sems.at[1],
            device_id=at(gx, j),
            device_id_type=MESH,
        ).start()
        return carry

    lax.fori_loop(1, span_y, send_load, 0)
    for k in range(planes):
        send_plane(k)

    def finish_plane(k, carry):
        wait_own(own_sem, k)
        wait_others(recv_sem, k)

        def split(r, carry):
            rows = pl.ds(pl.multiple_of(r * block, block), block)
            high[rows, :], low[rows, :] = halves(plane[k, rows, :])
            return carry

        lax.fori_loop(0, size_y // block, split, 0)

        def multiply(r, carry):
            rows = pl.ds(pl.multiple_of(r * block, block), block)
            along_y = dot3(cy_high[rows, :], cy_low[rows, :], high[...], low[...])
            y_high, y_low = halves(along_y)
            done[k, rows, :] = dot3(y_high, y_low, cx_high[...], cx_low[...])
            return carry

        lax.fori_loop(0, size_y // block, multiply, 0)
        send_back(k)
        return carry

    lax.fori_loop(0, planes, finish_plane, 0)
    some_loads = loads.at[pl.ds(0, span_y - 1)]
    pltpu.make_async_copy(some_loads, some_loads, load_sems.at[0]).wait()
    pltpu.make_async_copy(some_loads, some_loads, load_sems.at[1]).wait()
    own_load.wait()
    for k in range(planes):
        wait_others(send_sem, k)
        wait_others(back_send, k)
        wait_own(back_own, k)
        wait_others(back_recv, k)


def smooth(zfirst, loads, cy, cx, span_x, span_y):
    planes, devices, cells_y, cells_x = zfirst.shape
    size_y, size_x = cy.shape[0], cx.shape[0]
    anywhere = pl.BlockSpec(memory_space=pl.ANY)
    inside = pl.BlockSpec(memory_space=pltpu.VMEM)
    sems = pltpu.SemaphoreType.DMA((planes,))
    return pl.pallas_call(
        functools.partial(smooth_kernel, span_x, span_y),
        in_specs=[anywhere] * 2 + [inside] * 4,
        out_specs=[anywhere] * 2,
        out_shape=[
            jax.ShapeDtypeStruct(zfirst.shape, jnp.float32),
            jax.ShapeDtypeStruct(loads.shape, jnp.float32),
        ],
        scratch_shapes=[
            pltpu.VMEM((planes, size_y, size_x), jnp.float32),
            pltpu.VMEM((planes, size_y, size_x), jnp.float32),
            pltpu.VMEM((size_y, size_x), jnp.bfloat16),
            pltpu.VMEM((size_y, size_x), jnp.bfloat16),
        ]
        + [sems] * 6
        + [pltpu.SemaphoreType.DMA((3,))],
        compiler_params=pltpu.CompilerParams(
            collective_id=0, has_side_effects=True, vmem_limit_bytes=vmem_grant
        ),
        name="smooth",
    )(zfirst, loads, *outer_halves(cy), *outer_halves(cx))


def turn_kernel(source_ref, out_ref):
    for row in range(source_ref.shape[1]):
        out_ref[:, row, :] = source_ref[:, row, :].T


def turn(source):
    depth_all, cells_y, cells_x = source.shape
    rows = 8
    return pl.pallas_call(
        turn_kernel,
        grid=(cells_y // rows,),
        in_specs=[pl.BlockSpec((depth_all, rows, cells_x), lambda j: (0, j, 0))],
        out_specs=pl.BlockSpec((cells_x, rows, depth_all), lambda j: (0, j, 0)),
        out_shape=jax.ShapeDtypeStruct((cells_x, cells_y, depth_all), jnp.float32),
        name="turn",
    )(source)


def wave_freq(length):
    half = length // 2
    return jnp.concatenate(
        [jnp.arange(half + 1, dtype=jnp.int32), jnp.arange(1, half, dtype=jnp.int32)]
    )


def wave_table(length):
    half = length // 2
    indices = jnp.arange(length, dtype=jnp.int32)
    turns = indices[:, None] * wave_freq(length)[None, :] % length
    angles = 2.0 * math.pi / length * turns.astype(jnp.float32)
    shift = jnp.where(indices < half + 1, 0.0, math.pi / 2)[None, :]
    return lax.optimization_barrier(jnp.cos(angles - shift))


def circulant(gain, table):
    length = gain.shape[0]
    half = length // 2
    freq = wave_freq(length)
    weight = jnp.concatenate([gain[: half + 1], gain[1:half]])
    doubled = jnp.where((freq == 0) | (freq == half), 1.0, 2.0).astype(jnp.float32)
    scaled = lax.optimization_barrier(table * (weight * doubled / length))
    return lax.dot_general(
        scaled, table, (((1,), (1,)), ((), ())), precision=lax.Precision.HIGHEST
    )


def on_device(log_crit, col_bins, rate_table, tile_mask, tile_route, filt_x, filt_y):
    blocks_x, blocks_y, tiles = tile_mask.shape
    cells_x, cells_y, depth_all = log_crit.shape
    edge = cells_x // blocks_x
    span_x, span_y = lax.axis_size("gx"), lax.axis_size("gy")
    devices = span_x * span_y
    nodes = rate_table.shape[1]
    half = nodes // 2

    bins = col_bins.transpose(1, 2, 0).reshape(cells_y * tiles, cells_x)
    live = (tile_mask == 1).astype(jnp.float32).transpose(1, 2, 0)
    live = jnp.broadcast_to(
        live[:, None, :, :, None], (blocks_y, edge, tiles, blocks_x, edge)
    ).reshape(cells_y * tiles, cells_x)
    table = jnp.concatenate([rate_table[:, half:], rate_table[:, half - 1 :: -1]], axis=1).T

    recomb, zfirst, sums = evaluate(log_crit, bins, live, table, node_growth(nodes), tiles)

    tile_means = jnp.sum(
        sums.reshape(blocks_y, edge, tiles, blocks_x, edge), axis=(1, 4)
    ) / (edge * edge * edge)
    route = tile_route.transpose(1, 2, 0)
    capacity = blocks_x * blocks_y * tiles // 2
    route_ids = jnp.arange(span_y, dtype=jnp.int32)
    contribution = (
        jnp.sum(
            jnp.where(route[..., None] == route_ids, tile_means[..., None], 0.0), axis=(0, 1, 2)
        )
        / capacity
    )
    table_x = wave_table(filt_x.shape[0])
    table_y = table_x if filt_y.shape == filt_x.shape else wave_table(filt_y.shape[0])
    back, load_parts = smooth(
        zfirst.reshape(depth_all // devices, devices, cells_y, cells_x),
        jnp.broadcast_to(contribution[:, None, None], (span_y, 8, 128)),
        circulant(filt_y, table_y), circulant(filt_x, table_x), span_x, span_y,
    )
    device_load = jnp.sum(load_parts[:, 0, 0])
    smoothed = turn(back.reshape(depth_all, cells_y, cells_x))
    return (recomb, smoothed, device_load.reshape(1, 1))


def solution(mesh):
    placed = (
        P("gx", "gy", None),
        P("gx", "gy", None),
        P(),
        P("gx", "gy", None),
        P("gx", "gy", None),
        P(),
        P(),
    )
    return jax.shard_map(
        on_device,
        mesh=mesh,
        in_specs=placed,
        out_specs=(P("gx", "gy", None), P("gx", "gy", None), P("gx", "gy")),
        check_vma=False,
    )
```
